32 devices in a mesh: batch: 8 (over y, x, core), chan: 4 (over z).
Axes of the slice: x: 2, y: 2, z: 4, core: 2. Of those that a mesh axis runs over, the one named last changes fastest.
Arguments:
- images: bfloat16 [64, 14, 14, 4096], P('batch', None, None, 'chan'), may hold values from -12 to 12, as said below
- reduce_weight: bfloat16 [4096, 1024], P(None, 'chan'), may hold values from -0.09375 to 0.09375
- reduce_gain: float32 [1024], P('chan'), may hold values from 0.25 to 1.75
- reduce_bias: float32 [1024], P('chan'), may hold values from -0.5 to 0.5
- spatial_weight: bfloat16 [3, 3, 1024, 1024], P(None, None, None, 'chan'), may hold values from -0.0625 to 0.0625
- spatial_gain: float32 [1024], P('chan'), may hold values from 0.25 to 1.75
- spatial_bias: float32 [1024], P('chan'), may hold values from -0.5 to 0.5
- expand_weight: bfloat16 [1024, 4096], P(None, 'chan'), may hold values from -0.1875 to 0.1875
- expand_gain: float32 [4096], P('chan'), may hold values from 0.25 to 1.75
- expand_bias: float32 [4096], P('chan'), may hold values from -0.5 to 0.5
Outputs:
- block_out: bfloat16 [64, 14, 14, 4096], P('batch', None, None, 'chan')
The draws below stay inside these ranges and needn't reach their ends.
Inputs may be any that keep to these rules, and one draw needn't show every extreme that they name: In the images, the per-channel mean and scale differ from one block of 8 images to the next.
All inputs are finite; a program needn't handle non-finite values.
Results may differ from the reference program's by a relative error of at most 0.0047.
Values may be sent and summed in bfloat16 or wider, within the bound.
No kernel may reach another device: no remote copies, remote signals or barrier semaphores. Data moves between devices by JAX's collectives and lax.ppermute only.
A program may use at most 128 MiB of HBM per device.

```python
import jax
import jax.numpy as jnp
from jax import lax

CIN = 4096
MID = 1024
SIDE = 14
IMG_DEV = 8
IMAGES = 64


def draw_images(key, part):
    k_offset, k_scale, k_base = jax.random.split(jax.random.fold_in(key, 11), 3)
    groups = IMAGES // IMG_DEV
    offset = jnp.clip(1.5 * jax.random.normal(k_offset, (groups, 1, 1, 1, CIN), jnp.float32), -3.0, 3.0)
    scales = jnp.exp(jax.random.uniform(k_scale, (groups, 1, 1, 1, CIN), jnp.float32, -0.693, 0.693))
    shape = (groups, IMG_DEV, SIDE, SIDE, CIN)
    base = jnp.clip(jax.random.normal(k_base, shape, jnp.float32), -4.0, 4.0)
    values = jnp.clip(offset + scales * base, -12.0, 12.0)
    return values.reshape(IMAGES, SIDE, SIDE, CIN).astype(jnp.bfloat16)


def steps_of(key, shape, shards, least, top_value):
    level, own = 1.0, jax.random.fold_in(key, 6)
    for position, shards_of in shards:
        steps = jnp.exp(jax.random.uniform(jax.random.fold_in(own, position), (shards_of,), jnp.float32, least / len(shards), top_value / len(shards)))
        level = level * jnp.repeat(steps, shape[position] // shards_of).reshape([-1 if axis == position else 1 for axis in range(len(shape))])
    return level


def normal_values(rng, shape, spread, reach, cuts=(), dtype=jnp.bfloat16):
    level = steps_of(rng, shape, cuts, -0.22, 0.18) if cuts else 1.0
    array = jax.random.normal(rng, shape, jnp.float32) * spread * level
    return jnp.minimum(jnp.maximum(array, -reach), reach).astype(dtype)


def setup_inputs(seed: int = 0) -> dict:
    streams_of = jax.random.split(jax.random.key(seed), 11)
    images = draw_images(jax.random.fold_in(streams_of[10], 71), 0)
    reduce_weight = normal_values(streams_of[1], (CIN, MID), CIN ** -0.5, 0.09375, ((1, 4),))
    reduce_gain = jnp.clip(1.0 + 0.15 * jax.random.normal(streams_of[2], (MID,), jnp.float32), 0.25, 1.75)
    reduce_bias = jnp.clip(jax.random.uniform(streams_of[3], (MID,), jnp.float32, -0.5, 0.5) * steps_of(streams_of[3], (MID,), ((0, 4),), -0.4, 0.0), -0.5, 0.5)
    spatial_weight = normal_values(streams_of[4], (3, 3, MID, MID), (9 * MID) ** -0.5, 0.0625, ((3, 4),))
    spatial_gain = jnp.clip(1.0 + 0.15 * jax.random.normal(streams_of[5], (MID,), jnp.float32), 0.25, 1.75)
    spatial_bias = jnp.clip(jax.random.uniform(streams_of[6], (MID,), jnp.float32, -0.5, 0.5) * steps_of(streams_of[6], (MID,), ((0, 4),), -0.4, 0.0), -0.5, 0.5)
    expand_weight = normal_values(streams_of[7], (MID, CIN), MID ** -0.5, 0.1875, ((1, 4),))
    expand_gain = jnp.clip(1.0 + 0.15 * jax.random.normal(streams_of[8], (CIN,), jnp.float32), 0.25, 1.75)
    expand_bias = jnp.clip(jax.random.uniform(streams_of[9], (CIN,), jnp.float32, -0.5, 0.5) * steps_of(streams_of[9], (CIN,), ((0, 4),), -0.4, 0.0), -0.5, 0.5)
    return dict(images=images, reduce_weight=reduce_weight, reduce_gain=reduce_gain, reduce_bias=reduce_bias, spatial_weight=spatial_weight, spatial_gain=spatial_gain, spatial_bias=spatial_bias, expand_weight=expand_weight, expand_gain=expand_gain, expand_bias=expand_bias)


eps = 0.001

def batch_norm(values, gain, bias):
    mean = lax.optimization_barrier(jnp.mean(values, axis=(0, 1, 2)))
    centred = values - mean
    var = lax.optimization_barrier(jnp.mean(centred * centred, axis=(0, 1, 2)))
    return centred * (gain / jnp.sqrt(var + eps)) + bias

def pointwise(maps, weight):
    flat = maps.reshape(-1, maps.shape[-1])
    out = jnp.dot(flat, weight, preferred_element_type=jnp.float32)
    return out.reshape(maps.shape[:-1] + (weight.shape[1],))

def reference(images, reduce_weight, reduce_gain, reduce_bias, spatial_weight, spatial_gain, spatial_bias, expand_weight, expand_gain, expand_bias):
    first = pointwise(images, reduce_weight)
    act_one = jnp.maximum(batch_norm(first, reduce_gain, reduce_bias), 0.0).astype(jnp.bfloat16)
    padded = jnp.pad(act_one, ((0, 0), (1, 1), (1, 1), (0, 0)))
    second = jnp.zeros(act_one.shape[:-1] + (spatial_weight.shape[3],), jnp.float32)
    for row_tap in range(3):
        for col_tap in range(3):
            window = padded[:, row_tap:row_tap + SIDE, col_tap:col_tap + SIDE, :]
            second = second + pointwise(window, spatial_weight[row_tap, col_tap])
    act_two = jnp.maximum(batch_norm(second, spatial_gain, spatial_bias), 0.0).astype(jnp.bfloat16)
    third = pointwise(act_two, expand_weight)
    summed = batch_norm(third, expand_gain, expand_bias) + images.astype(jnp.float32)
    return jnp.maximum(summed, 0.0).astype(jnp.bfloat16)
```

```python
import jax
import jax.numpy as jnp
from jax import lax
from jax.sharding import PartitionSpec as P

eps = 0.001


def send(value, shift):
    size = lax.axis_size("chan")
    return lax.ppermute(value, "chan", [(k, (k + shift) % size) for k in range(size)])


def pass_on(value, step, senders):
    return lax.ppermute(value, "chan", [(k, k + step) for k in senders])


def rows_for_others(weight, channels):
    size, me = lax.axis_size("chan"), lax.axis_index("chan")
    width = lax.axis_size("batch")
    share = 2 if width % 2 == 0 else 1
    part = lax.rem(lax.axis_index("batch"), share)
    height = channels // share
    found = {}
    for shift in range(1, size):
        owner = lax.rem(me - shift + size, size)
        half = lax.dynamic_slice_in_dim(weight, owner * channels + part * height, height, 0)
        got = send(half, size - shift)
        if share == 1:
            found[shift] = got
            continue
        other = lax.ppermute(got, "batch", [(k, k ^ 1) for k in range(width)])
        found[shift] = (got, other)
    return found, part, height


def reduce_blocks(flat, weight):
    channels = flat.shape[1]
    size, me = lax.axis_size("chan"), lax.axis_index("chan")
    found, part, height = rows_for_others(weight, channels)
    own = lax.dynamic_slice_in_dim(weight, me * channels, channels, 0)
    total = jnp.dot(flat, own, preferred_element_type=jnp.float32)
    terms = {}
    for shift, got in found.items():
        if isinstance(got, tuple):
            first = part == 0
            got = jnp.concatenate(
                [jnp.where(first, got[0], got[1]), jnp.where(first, got[1], got[0])], axis=0
            )
        terms[shift] = jnp.dot(flat, got, preferred_element_type=jnp.float32)
    right = left = None
    for far in range(size - 1, 0, -1):
        to_right, to_left = terms[far], terms[size - far]
        if right is not None:
            to_right = to_right + right.astype(jnp.float32)
            to_left = to_left + left.astype(jnp.float32)
        right = pass_on(to_right.astype(jnp.bfloat16), 1, range(size - far))
        left = pass_on(to_left.astype(jnp.bfloat16), -1, range(far, size))
    if right is None:
        return total
    return total + (right.astype(jnp.float32) + left.astype(jnp.float32))


def centre(values):
    mean = jnp.sum(values, axis=0) / values.shape[0]
    centred = values - mean
    return centred, mean, jnp.sum(centred * centred, axis=0)


def affine(mean, spread, gain, bias, rows):
    each = lax.all_gather(jnp.stack([mean, spread]), "batch")
    total_mean = jnp.mean(each[:, 0], axis=0)
    away = each[:, 0] - total_mean
    var = (jnp.sum(each[:, 1], axis=0) / rows + jnp.sum(away * away, axis=0)) / each.shape[0]
    scale = gain / jnp.sqrt(var + eps)
    return jnp.stack([scale, bias + (mean - total_mean) * scale])


def activation(centred, pair):
    return jnp.maximum(centred.astype(jnp.float32) * pair[0] + pair[1], 0.0).astype(jnp.bfloat16)


def spread_blocks(values, gain, bias):
    size, me = lax.axis_size("chan"), lax.axis_index("chan")
    centred, mean, spread = centre(values)
    packed = centred.astype(jnp.bfloat16)
    right, left = {0: packed}, {0: packed}
    for step in range(1, size):
        right[step] = pass_on(right[step - 1], 1, range(step - 1, size - 1))
        left[step] = pass_on(left[step - 1], -1, range(1, size - step + 1))
    pair = affine(mean, spread, gain, bias, values.shape[0])
    result = [(me, activation(centred, pair))]
    for step in sorted(range(1, size), key=lambda step: max(step, size - step)):
        owner = lax.rem(me - step + size, size)
        block = jnp.where(me >= step, right[step], left[size - step])
        result.append((owner, activation(block, send(pair, step))))
    return result


def body(
    images,
    reduce_weight,
    reduce_gain,
    reduce_bias,
    spatial_weight,
    spatial_gain,
    spatial_bias,
    expand_weight,
    expand_gain,
    expand_bias,
):
    imgs, side, channels = images.shape[0], images.shape[1], images.shape[3]
    rows = imgs * side * side
    mid = reduce_weight.shape[1]
    size, me = lax.axis_size("chan"), lax.axis_index("chan")

    flat = jnp.transpose(images, (1, 2, 0, 3)).reshape(rows, channels)
    first = reduce_blocks(flat, reduce_weight)

    second = None
    for owner, block in spread_blocks(first, reduce_gain, reduce_bias):
        weight = lax.dynamic_slice_in_dim(spatial_weight, owner * mid, mid, 2)
        term = lax.conv_general_dilated(
            block.reshape(side, side, imgs, mid),
            weight,
            (1, 1),
            ((1, 1), (1, 1)),
            dimension_numbers=("HWNC", "HWIO", "HWNC"),
            preferred_element_type=jnp.float32,
        )
        second = term if second is None else second + term
    second = second.reshape(rows, mid)

    third = None
    for owner, block in spread_blocks(second, spatial_gain, spatial_bias):
        weight = lax.dynamic_slice_in_dim(expand_weight, owner * mid, mid, 0)
        term = jnp.dot(block, weight, preferred_element_type=jnp.float32)
        third = term if third is None else third + term

    centred, mean, spread = centre(third)
    pair = affine(mean, spread, expand_gain, expand_bias, rows)
    summed = centred * pair[0] + pair[1] + flat.astype(jnp.float32)
    out = jnp.maximum(summed, 0.0).astype(jnp.bfloat16)
    return jnp.transpose(out.reshape(side, side, imgs, channels), (2, 0, 1, 3))


def solution(mesh):
    in_specs = (
        P("batch", None, None, "chan"),
        P(None, "chan"),
        P("chan"),
        P("chan"),
        P(None, None, None, "chan"),
        P("chan"),
        P("chan"),
        P(None, "chan"),
        P("chan"),
        P("chan"),
    )
    out_specs = P("batch", None, None, "chan")
    return jax.shard_map(body, mesh=mesh, in_specs=in_specs, out_specs=out_specs, check_vma=False)
```

```python
import jax
import jax.numpy as jnp
from jax import lax
from jax.sharding import PartitionSpec as P

eps = 0.001


def send(value, shift):
    size = lax.axis_size("chan")
    return lax.ppermute(value, "chan", [(k, (k + shift) % size) for k in range(size)])


def pass_on(value, step, senders):
    return lax.ppermute(value, "chan", [(k, k + step) for k in senders])


def rows_for_others(weight, channels):
    size, me = lax.axis_size("chan"), lax.axis_index("chan")
    width = lax.axis_size("batch")
    share = 2 if width % 2 == 0 else 1
    part = lax.rem(lax.axis_index("batch"), share)
    height = channels // share
    halves = []
    for shift in range(1, size):
        owner = lax.rem(me - shift + size, size)
        half = lax.dynamic_slice_in_dim(weight, owner * channels + part * height, height, 0)
        halves.append(send(half, size - shift))
    halves = lax.optimization_barrier(halves)
    if share == 1:
        return dict(enumerate(halves, 1)), part, height
    others = [lax.ppermute(half, "batch", [(k, k ^ 1) for k in range(width)]) for half in halves]
    halves, others = lax.optimization_barrier((halves, others))
    found = {shift: pair for shift, pair in enumerate(zip(halves, others), 1)}
    return found, part, height


def reduce_blocks(flat, weight):
    channels = flat.shape[1]
    size, me = lax.axis_size("chan"), lax.axis_index("chan")
    found, part, height = rows_for_others(weight, channels)
    own = lax.dynamic_slice_in_dim(weight, me * channels, channels, 0)
    total = jnp.dot(flat, own, preferred_element_type=jnp.float32)
    terms = {}
    for shift, got in found.items():
        if isinstance(got, tuple):
            first = part == 0
            got = jnp.concatenate(
                [jnp.where(first, got[0], got[1]), jnp.where(first, got[1], got[0])], axis=0
            )
        terms[shift] = jnp.dot(flat, got, preferred_element_type=jnp.float32)
    terms = lax.optimization_barrier(terms)
    right = left = None
    for far in range(size - 1, 0, -1):
        to_right, to_left = terms[far], terms[size - far]
        if right is not None:
            to_right = to_right + right.astype(jnp.float32)
            to_left = to_left + left.astype(jnp.float32)
        right = pass_on(to_right.astype(jnp.bfloat16), 1, range(size - far))
        left = pass_on(to_left.astype(jnp.bfloat16), -1, range(far, size))
        right, left = lax.optimization_barrier((right, left))
    if right is None:
        return total
    return total + (right.astype(jnp.float32) + left.astype(jnp.float32))


def centre(values):
    mean = jnp.sum(values, axis=0) / values.shape[0]
    centred = values - mean
    return centred, mean, jnp.sum(centred * centred, axis=0)


def affine(mean, spread, gain, bias, rows):
    each = lax.all_gather(jnp.stack([mean, spread]), "batch")
    total_mean = jnp.mean(each[:, 0], axis=0)
    away = each[:, 0] - total_mean
    var = (jnp.sum(each[:, 1], axis=0) / rows + jnp.sum(away * away, axis=0)) / each.shape[0]
    scale = gain / jnp.sqrt(var + eps)
    return jnp.stack([scale, bias + (mean - total_mean) * scale])


def activation(centred, pair):
    return jnp.maximum(centred.astype(jnp.float32) * pair[0] + pair[1], 0.0).astype(jnp.bfloat16)


def spread_blocks(values, gain, bias):
    size, me = lax.axis_size("chan"), lax.axis_index("chan")
    centred, mean, spread = centre(values)
    packed = centred.astype(jnp.bfloat16)
    right, left = {0: packed}, {0: packed}
    for step in range(1, size):
        right[step] = pass_on(right[step - 1], 1, range(step - 1, size - 1))
        left[step] = pass_on(left[step - 1], -1, range(1, size - step + 1))
    pair = affine(mean, spread, gain, bias, values.shape[0])
    result = [(me, activation(centred, pair))]
    for step in sorted(range(1, size), key=lambda step: max(step, size - step)):
        owner = lax.rem(me - step + size, size)
        block = jnp.where(me >= step, right[step], left[size - step])
        result.append((owner, activation(block, send(pair, step))))
    return result


def body(
    images,
    reduce_weight,
    reduce_gain,
    reduce_bias,
    spatial_weight,
    spatial_gain,
    spatial_bias,
    expand_weight,
    expand_gain,
    expand_bias,
):
    imgs, side, channels = images.shape[0], images.shape[1], images.shape[3]
    rows = imgs * side * side
    mid = reduce_weight.shape[1]
    size, me = lax.axis_size("chan"), lax.axis_index("chan")

    flat = jnp.transpose(images, (1, 2, 0, 3)).reshape(rows, channels)
    first = reduce_blocks(flat, reduce_weight)

    second = None
    for owner, block in spread_blocks(first, reduce_gain, reduce_bias):
        weight = lax.dynamic_slice_in_dim(spatial_weight, owner * mid, mid, 2)
        term = lax.conv_general_dilated(
            block.reshape(side, side, imgs, mid),
            weight,
            (1, 1),
            ((1, 1), (1, 1)),
            dimension_numbers=("HWNC", "HWIO", "HWNC"),
            preferred_element_type=jnp.float32,
        )
        second = term if second is None else second + term
    second = second.reshape(rows, mid)

    third = None
    for owner, block in spread_blocks(second, spatial_gain, spatial_bias):
        weight = lax.dynamic_slice_in_dim(expand_weight, owner * mid, mid, 0)
        term = jnp.dot(block, weight, preferred_element_type=jnp.float32)
        third = term if third is None else third + term

    centred, mean, spread = centre(third)
    pair = affine(mean, spread, expand_gain, expand_bias, rows)
    summed = centred * pair[0] + pair[1] + flat.astype(jnp.float32)
    out = jnp.maximum(summed, 0.0).astype(jnp.bfloat16)
    return jnp.transpose(out.reshape(side, side, imgs, channels), (2, 0, 1, 3))


def solution(mesh):
    in_specs = (
        P("batch", None, None, "chan"),
        P(None, "chan"),
        P("chan"),
        P("chan"),
        P(None, None, None, "chan"),
        P("chan"),
        P("chan"),
        P(None, "chan"),
        P("chan"),
        P("chan"),
    )
    out_specs = P("batch", None, None, "chan")
    return jax.shard_map(body, mesh=mesh, in_specs=in_specs, out_specs=out_specs, check_vma=False)
```
